64 devices in a mesh: prob: 4 (over x, y), feat: 16 (over z, core).
Axes of the slice: x: 2, y: 2, z: 8, core: 2. Of those that a mesh axis runs over, the one named last changes fastest.
The devices are a block of a 4x4x8 slice.
Arguments:
- x_mat: bfloat16 [32768, 16384], P('prob', 'feat'), parts along dimension 0
- w_init: float32 [65536, 2, 100], P(('prob', 'feat')), parts along dimension 0
- y_targ: float32 [32768, 2, 100], P('prob'), parts along dimension 0
- step_eta: float32 [65536], P(('prob', 'feat')), parts along dimension 0
Outputs:
- output 1: float32 [65536, 2, 100], P(('prob', 'feat')), parts along dimension 0
- output 2: float32 [32768, 2, 100], P('prob'), parts along dimension 0
There are 4 independent parts. The reference program is written for one: setup_inputs(seed, part) draws one part's arguments, and reference() takes and returns one part's arrays. A program takes and returns all parts, laid end to end along the dimension named above; each array names one.
All inputs are finite; a program needn't handle non-finite values.
Results may differ from the reference program's by a relative error of at most 0.00406533.
Values are sent between devices in bfloat16 or wider.
A program may use at most 768 MiB of HBM per device.

```python
import jax
import jax.numpy as jnp
from jax import lax

SAMPLES = 8192
FEAT_DEV = 1024
GROUP_SIZE = 16
TARGETS = 100
SWEEPS = 4
LOW_RANK = 8
FEATURES = FEAT_DEV * GROUP_SIZE


def setup_inputs(seed: int = 0, part: int = 0) -> dict:
    root_key = jax.random.key(seed)
    part_key = jax.random.fold_in(root_key, part)
    sub_keys = jax.random.split(part_key, 7)
    iid_noise = jax.random.normal(sub_keys[0], (SAMPLES, FEATURES), jnp.float32)
    factors = jax.random.normal(sub_keys[1], (SAMPLES, LOW_RANK), jnp.float32)
    loadings = jax.random.normal(sub_keys[2], (LOW_RANK, FEATURES), jnp.float32) * (2.0 / SAMPLES) ** 0.5
    x_mat = (iid_noise + jnp.dot(factors, loadings)).astype(jnp.bfloat16)
    col_sq = jnp.sum(jnp.square(x_mat.astype(jnp.float32)), axis=0) / SAMPLES
    spread = jax.random.uniform(sub_keys[3], (FEATURES,), jnp.float32, 0.4, 1.2)
    step_eta = spread / (GROUP_SIZE * col_sq)
    w_true = jax.random.normal(sub_keys[4], (FEATURES, 2 * TARGETS), jnp.float32) * FEATURES ** -0.5
    w_init = jax.random.normal(sub_keys[5], (FEATURES, 2, TARGETS), jnp.float32) * (0.8 * FEATURES ** -0.5)
    y_clean = jnp.dot(x_mat, w_true.astype(jnp.bfloat16), preferred_element_type=jnp.float32)
    y_noise = 0.5 * jax.random.normal(sub_keys[6], (SAMPLES, 2 * TARGETS), jnp.float32)
    y_targ = (y_clean + y_noise).reshape(SAMPLES, 2, TARGETS)
    return {"x_mat": x_mat, "w_init": w_init, "y_targ": y_targ, "step_eta": step_eta}


def reference(x_mat, w_init, y_targ, step_eta):
    ridge_wt = jnp.array([0.1, 1.0], jnp.float32).reshape(1, 2, 1)
    eta_col = step_eta.reshape(FEATURES, 1, 1)

    def block_sum(w_cur):
        w_blocks = w_cur.astype(jnp.bfloat16).reshape(GROUP_SIZE, FEAT_DEV, 2 * TARGETS)

        def add_block(running, block_pair):
            block_idx, w_block = block_pair
            x_block = lax.dynamic_slice_in_dim(x_mat, block_idx * FEAT_DEV, FEAT_DEV, axis=1)
            part_prod = jnp.dot(x_block, w_block, preferred_element_type=jnp.float32).astype(jnp.bfloat16)
            return running + part_prod.astype(jnp.float32), None

        start_sum = jnp.zeros((SAMPLES, 2 * TARGETS), jnp.float32)
        summed, no_out = lax.scan(add_block, start_sum, (jnp.arange(GROUP_SIZE), w_blocks))
        return summed.reshape(SAMPLES, 2, TARGETS)

    def one_sweep(state_pair, unused):
        w_cur, residual = state_pair
        r_half = residual.astype(jnp.bfloat16).reshape(SAMPLES, 2 * TARGETS)
        gradient = jnp.dot(x_mat.T, r_half, preferred_element_type=jnp.float32).reshape(FEATURES, 2, TARGETS) / SAMPLES
        w_step = eta_col * (gradient - ridge_wt * w_cur)
        return (w_cur + w_step, residual - block_sum(w_step)), None

    start_resid = y_targ - block_sum(w_init)
    final_pair, no_out = lax.scan(one_sweep, (w_init, start_resid), None, length=SWEEPS)
    w_out, r_out = final_pair
    return w_out, r_out
```

```python
import functools

import jax
import jax.numpy as jnp
from jax import lax
from jax.experimental import pallas as pl
from jax.experimental.pallas import tpu as pltpu
from jax.sharding import PartitionSpec as P

SWEEPS = 4
MESH = pl.DeviceIdType.MESH


def _kernel(cfg, x_in, w_in, eta_in, y_in, w_res, r_res,
            xo, xp, pf, rup, rdn, gat, w, g, dwb, eta, res, rf,
            xo_sem, xs_sem, xr_sem, in_sem,
            rsu_s, rsu_r, rsd_s, rsd_r,
            agu_s, agu_r, agd_s, agd_r,
            fgu_s, fgu_r, fgd_s, fgd_r,
            po_s, po_r, lo_s, wo_sem):
    Z, KP, KB, H, DP, N, lams = cfg
    hops = Z - 1
    half_ring = Z // 2
    me = lax.axis_index("feat")
    z = lax.div(me, 2)
    c = lax.rem(me, 2)
    up = {"feat": lax.rem(z + 1, Z) * 2 + c}
    dn = {"feat": lax.rem(z + Z - 1, Z) * 2 + c}
    pal = {"feat": me + 1 - 2 * c}

    def chunk(off, half):
        return lax.rem(z + off + Z, Z) * 2 + half

    def up_chunk(m):
        return chunk(half_ring - lax.div(m + 1, 2), lax.rem(m, 2))

    def dn_chunk(m):
        return chunk(lax.div(m + 1, 2) - half_ring, 1 - lax.rem(m, 2))

    def remote(src, dst, ss, rs, dev):
        return pltpu.make_async_remote_copy(src_ref=src, dst_ref=dst, send_sem=ss, recv_sem=rs,
                                            device_id=dev, device_id_type=MESH)

    local = pltpu.make_async_copy

    in_copies = [local(w_in.at[c], w.at[0], in_sem.at[0]),
                 local(eta_in, eta.at[0], in_sem.at[1]),
                 local(y_in, res, in_sem.at[2])]
    for cp in in_copies:
        cp.start()

    def xo_copy(k):
        return local(x_in.at[k], xo.at[k], xo_sem.at[k])

    def xp_copy(k):
        return remote(x_in.at[k], xp.at[k], xs_sem.at[k], xr_sem.at[k], pal)

    def start_xo(m, _):
        xo_copy(up_chunk(m)).start()
        xo_copy(dn_chunk(m)).start()
        return 0
    lax.fori_loop(0, Z, start_xo, 0)

    bar = pltpu.get_barrier_semaphore()
    for dev in (up, dn, pal):
        pl.semaphore_signal(bar, inc=1, device_id=dev, device_id_type=MESH)
    pl.semaphore_wait(bar, 3)

    w_x = remote(w_in.at[1 - c], w.at[1], in_sem.at[3], in_sem.at[4], pal)
    e_x = remote(eta_in, eta.at[1], in_sem.at[5], in_sem.at[6], pal)
    w_x.start()
    e_x.start()

    def start_xp(m, _):
        xp_copy(up_chunk(m)).start()
        xp_copy(dn_chunk(m)).start()
        return 0
    lax.fori_loop(0, Z, start_xp, 0)

    for cp in in_copies:
        cp.wait()
    w_x.wait()
    e_x.wait()

    def to_half(v):
        return jnp.concatenate([v, jnp.zeros((KB - KP, v.shape[1]), jnp.float32)], axis=0).astype(jnp.bfloat16)

    for b in range(2):
        dwb[b] = to_half(w[b])

    CB = 256

    def product(k):
        for j in range(H // CB if H >= CB else 1):
            cols = pl.ds(j * CB, min(CB, H))
            total = None
            for b, xx in ((0, xo), (1, xp)):
                part = lax.dot_general(dwb[b], xx[k, cols, :], (((1,), (1,)), ((), ())),
                                       preferred_element_type=jnp.float32)
                part = part.astype(jnp.bfloat16).astype(jnp.float32)
                total = part if total is None else total + part
            pf[k, :, cols] = total[:KP]

    def gradient(k):
        rows = gat[k]
        for b, xx in ((0, xo), (1, xp)):
            for j in range(DP // CB):
                cols = pl.ds(j * CB, CB)
                part = jnp.dot(rows, xx[k, :, cols], preferred_element_type=jnp.float32)
                g[b, :, cols] += part[:KP]

    def rs_up(m, src):
        return remote(src, rup.at[m], rsu_s.at[m], rsu_r.at[m], up)

    def rs_dn(m, src):
        return remote(src, rdn.at[m], rsd_s.at[m], rsd_r.at[m], dn)

    def ring_step(m, t, with_recv, with_send):
        ku, kd = up_chunk(m), dn_chunk(m)

        @pl.when(t == 0)
        def _():
            for k in (ku, kd):
                xo_copy(k).wait()
                xp_copy(k).wait_recv()
        product(ku)
        if with_send and not with_recv:
            rs_up(m, pf.at[ku]).start()
        product(kd)
        if with_send and not with_recv:
            rs_dn(m, pf.at[kd]).start()
        if with_recv:
            s = m - 2
            rs_up(s, rup.at[s]).wait_recv()
            rup[s] += pf[ku]
            rs_up(m, rup.at[s]).start()
            rs_dn(s, rdn.at[s]).wait_recv()
            rdn[s] += pf[kd]
            rs_dn(m, rdn.at[s]).start()

    def reduce_round(t):
        def first(m, _):
            ring_step(m, t, False, True)
            return 0

        def rest(m, _):
            ring_step(m, t, True, True)
            return 0
        lax.fori_loop(0, 2, first, 0)
        lax.fori_loop(2, hops, rest, 0)
        ring_step(hops, t, False, False)
        g[...] = jnp.zeros_like(g)
        a, b = hops - 2, hops - 1
        rs_up(a, rup.at[a]).wait_recv()
        rs_dn(a, rdn.at[a]).wait_recv()
        rs_up(b, rup.at[b]).wait_recv()
        k0, k1 = chunk(0, 0), chunk(0, 1)
        res[0] = res[0] - (rup[b] + rdn[a] + pf[k0])
        rs_dn(b, rdn.at[b]).wait_recv()
        res[1] = res[1] - (rup[a] + rdn[b] + pf[k1])

        def drain(m, _):
            rs_up(m, rup.at[m]).wait_send()
            rs_dn(m, rdn.at[m]).wait_send()
            return 0
        lax.fori_loop(0, hops, drain, 0)

    def gather_ring(buf, us, ur, ds, dr, seen):
        def send_up(m, k):
            return remote(buf.at[k], buf.at[k], us.at[m], ur.at[m], up)

        def send_dn(m, k):
            return remote(buf.at[k], buf.at[k], ds.at[m], dr.at[m], dn)
        k0, k1 = chunk(0, 0), chunk(0, 1)
        send_up(0, k0).start()
        send_dn(0, k1).start()
        send_up(1, k1).start()
        send_dn(1, k0).start()
        seen(k0)
        seen(k1)

        def step(m, _):
            far = lax.div(m, 2) + 1
            ku, kd = chunk(-far, lax.rem(m, 2)), chunk(far, 1 - lax.rem(m, 2))
            send_up(m, ku).wait_recv()

            @pl.when(m < hops - 2)
            def _():
                send_up(m + 2, ku).start()
            send_dn(m, kd).wait_recv()

            @pl.when(m < hops - 2)
            def _():
                send_dn(m + 2, kd).start()
            seen(ku)
            seen(kd)
            return 0
        lax.fori_loop(0, hops, step, 0)

        def drain(m, _):
            send_up(m, k0).wait_send()
            send_dn(m, k0).wait_send()
            return 0
        lax.fori_loop(0, hops, drain, 0)

    lam = jnp.where(c == 0, jnp.float32(lams[0]), jnp.float32(lams[1]))

    def one_round(t, _):
        reduce_round(t)

        @pl.when(t < SWEEPS)
        def _():
            for h in range(2):
                gat[chunk(0, h)] = to_half(res[h])
            gather_ring(gat, agu_s, agu_r, agd_s, agd_r, gradient)
            for b in range(2):
                for j in range(DP // CB):
                    cols = pl.ds(j * CB, CB)
                    old = w[b, :, cols]
                    step = eta[b, 0:1, cols] * (g[b, :, cols] * (1.0 / N) - lam * old)
                    w[b, :, cols] = old + step
                    dwb[b, :, cols] = to_half(step)
        return 0

    lax.fori_loop(0, SWEEPS + 1, one_round, 0)

    w_own = local(w.at[0], w_res.at[c], wo_sem.at[0])
    w_pal = remote(w.at[1], w_res.at[c], wo_sem.at[1], wo_sem.at[2], pal)
    w_own.start()
    w_pal.start()
    for h in range(2):
        rf[chunk(0, h)] = res[h]

    def out_local(k):
        return local(rf.at[k], r_res.at[c, k], lo_s.at[k])

    def out_pal(k):
        return remote(rf.at[k], r_res.at[c, k], po_s.at[k], po_r.at[k], pal)

    def emit(k):
        out_pal(k).start()
        out_local(k).start()
    gather_ring(rf, fgu_s, fgu_r, fgd_s, fgd_r, emit)

    def finish(k, _):
        out_local(k).wait()
        out_pal(k).wait()
        xp_copy(k).wait_send()
        return 0
    lax.fori_loop(0, 2 * Z, finish, 0)
    w_own.wait()
    w_pal.wait()


def _fused(x, wt, eta, ysh, Z, KP, KB, H, DP, N):
    hops = Z - 1
    any_spec = pl.BlockSpec(memory_space=pl.ANY)
    f32, b16 = jnp.float32, jnp.bfloat16
    dma = pltpu.SemaphoreType.DMA
    cfg = (Z, KP, KB, H, DP, N, (0.1, 1.0))
    scratch = [
        pltpu.VMEM((2 * Z, H, DP), b16), pltpu.VMEM((2 * Z, H, DP), b16),
        pltpu.VMEM((2 * Z, KP, H), f32),
        pltpu.VMEM((hops, KP, H), f32), pltpu.VMEM((hops, KP, H), f32),
        pltpu.VMEM((2 * Z, KB, H), b16),
        pltpu.VMEM((2, KP, DP), f32), pltpu.VMEM((2, KP, DP), f32), pltpu.VMEM((2, KB, DP), b16),
        pltpu.VMEM((2, 8, DP), f32), pltpu.VMEM((2, KP, H), f32),
        pltpu.VMEM((2 * Z, KP, H), f32),
        dma((2 * Z,)), dma((2 * Z,)), dma((2 * Z,)), dma((7,)),
    ] + [dma((hops,))] * 12 + [dma((2 * Z,)), dma((2 * Z,)), dma((2 * Z,)), dma((3,))]
    flops = (SWEEPS * 2 + 1) * 2 * N * DP * 2 * KP
    return pl.pallas_call(
        functools.partial(_kernel, cfg),
        out_shape=(jax.ShapeDtypeStruct((2, KP, DP), f32), jax.ShapeDtypeStruct((2, 2 * Z, KP, H), f32)),
        in_specs=[any_spec] * 4,
        out_specs=(any_spec, any_spec),
        scratch_shapes=scratch,
        compiler_params=pltpu.CompilerParams(collective_id=0, has_side_effects=True, vmem_limit_bytes=64000000),
        cost_estimate=pl.CostEstimate(flops=flops, bytes_accessed=2 * N * DP * 2, transcendentals=0),
    )(x, wt, eta, ysh)


def solution(mesh):
    Z = mesh.shape["feat"] // 2

    def per_device(x_blk, w_blk, y_blk, eta_blk):
        N, DP = x_blk.shape
        K = y_blk.shape[2]
        KP = -(-K // 8) * 8
        KB = -(-K // 16) * 16
        H = N // (2 * Z)
        me = lax.axis_index("feat")
        z, c = me // 2, me % 2
        wt = jnp.pad(jnp.transpose(w_blk, (1, 2, 0)), ((0, 0), (0, KP - K), (0, 0)))
        ysh = lax.dynamic_slice(y_blk, (z * 2 * H, c, 0), (2 * H, 1, K)).reshape(2, H, K)
        ysh = jnp.pad(jnp.transpose(ysh, (0, 2, 1)), ((0, 0), (0, KP - K), (0, 0)))
        eta = jnp.broadcast_to(eta_blk[None, :], (8, DP))
        w_t, r_t = _fused(x_blk.reshape(2 * Z, H, DP), wt, eta, ysh, Z, KP, KB, H, DP, N)
        w_new = jnp.transpose(w_t[:, :K, :], (2, 0, 1))
        r_new = jnp.transpose(r_t[:, :, :K, :], (1, 3, 0, 2)).reshape(N, 2, K)
        return w_new, r_new

    x_spec = P("prob", "feat")
    w_spec = P(("prob", "feat"), None, None)
    y_spec = P("prob", None, None)
    e_spec = P(("prob", "feat"))
    return jax.shard_map(per_device, mesh=mesh, in_specs=(x_spec, w_spec, y_spec, e_spec),
                         out_specs=(w_spec, y_spec), check_vma=False)
```

```python
import functools

import jax
import jax.numpy as jnp
from jax import lax
from jax.experimental import pallas as pl
from jax.experimental.pallas import tpu as pltpu
from jax.sharding import PartitionSpec as P

SWEEPS = 4
LAMS = (0.1, 1.0)
STAGGER = 2
MESH = pl.DeviceIdType.MESH


def _kernel(cfg, x_in, w_in, eta_in, y_in, w_res, r_res,
            xo, xp, pf, rup, rdn, gat, w, g, dwb, eta, res, rf,
            xo_sem, xs_sem, xr_sem, in_sem,
            rsu_s, rsu_r, rsd_s, rsd_r,
            agu_s, agu_r, agd_s, agd_r,
            fgu_s, fgu_r, fgd_s, fgd_r,
            po_s, po_r, lo_s, wo_sem, raw, yraw, flat, go_sem):
    Z, KS, KP, KB, H, DP, N = cfg
    K = w_in.shape[0]
    hops = Z - 1
    half_ring = Z // 2
    me = lax.axis_index("feat")
    z = lax.div(me, 2)
    c = lax.rem(me, 2)
    up = {"feat": lax.rem(z + 1, Z) * 2 + c}
    dn = {"feat": lax.rem(z + Z - 1, Z) * 2 + c}
    pal = {"feat": me + 1 - 2 * c}

    def chunk(off, half):
        return lax.rem(z + off + Z, Z) * 2 + half

    def up_chunk(m):
        return chunk(half_ring - lax.div(m + 1, 2), lax.rem(m, 2))

    def dn_chunk(m):
        return chunk(lax.div(m + 1, 2) - half_ring, 1 - lax.rem(m, 2))

    def remote(src, dst, ss, rs, dev):
        return pltpu.make_async_remote_copy(src_ref=src, dst_ref=dst, send_sem=ss, recv_sem=rs,
                                            device_id=dev, device_id_type=MESH)

    class Split:
        def __init__(self, make):
            self.make = make

        def do(self, act):
            @pl.when(c == 0)
            def _():
                act(self.make(0))

            @pl.when(c == 1)
            def _():
                act(self.make(1))

        def start(self):
            self.do(lambda cp: cp.start())

        def wait(self):
            self.do(lambda cp: cp.wait())

        def wait_send(self):
            self.do(lambda cp: cp.wait_send())

        def wait_recv(self):
            self.do(lambda cp: cp.wait_recv())

    rows32 = (pl.ds(0, KS), pl.ds(0, KP))
    rows16 = (pl.ds(0, KS), pl.ds(0, KB))
    rows_out = (pl.ds(0, KS), pl.ds(KS, KP))

    local = pltpu.make_async_copy

    y_cols = pl.ds(pl.multiple_of(z * (2 * H), 2 * H), 2 * H)
    in_copies = [local(w_in, raw.at[0], in_sem.at[0]),
                 local(eta_in, eta.at[0], in_sem.at[1]),
                 local(y_in.at[:, :, y_cols], yraw, in_sem.at[2])]
    for cp in in_copies:
        cp.start()

    def xo_copy(k):
        return local(x_in.at[k], xo.at[k], xo_sem.at[k])

    def xp_copy(k):
        return remote(x_in.at[k], xp.at[k], xs_sem.at[k], xr_sem.at[k], pal)

    def start_xo(m, _):
        xo_copy(up_chunk(m)).start()
        xo_copy(dn_chunk(m)).start()
        return 0
    lax.fori_loop(0, Z, start_xo, 0)

    bar = pltpu.get_barrier_semaphore()
    for dev in (up, dn, pal):
        pl.semaphore_signal(bar, inc=1, device_id=dev, device_id_type=MESH)
    pl.semaphore_wait(bar, 3)

    w_x = remote(w_in, raw.at[1], in_sem.at[3], in_sem.at[4], pal)
    e_x = remote(eta_in, eta.at[1], in_sem.at[5], in_sem.at[6], pal)
    w_x.start()
    e_x.start()

    def start_xp(m, _):
        xp_copy(up_chunk(m)).start()
        xp_copy(dn_chunk(m)).start()
        return 0
    lax.fori_loop(0, Z, start_xp, 0)

    for cp in in_copies:
        cp.wait()
    w_x.wait()
    e_x.wait()

    def to_half(v):
        return jnp.concatenate([v, jnp.zeros((KB - KP, v.shape[1]), jnp.float32)], axis=0).astype(jnp.bfloat16)

    mine = pl.ds(pl.multiple_of(c * KS, 8), KP)

    def flatten(src):
        wide = src.shape[2]
        flat[0:K, 0:wide] = src[:, 0, :]
        flat[K:2 * K, 0:wide] = src[:, 1, :]

    for b in range(2):
        flatten(raw.at[b])
        w[b] = flat[mine, 0:DP]
        dwb[b] = to_half(w[b])
    flatten(yraw)
    for h in range(2):
        res[h] = flat[mine, h * H:(h + 1) * H]

    @pl.when(c == 1)
    def _():
        pl.semaphore_wait(go_sem, 1)

    CB = 256

    def product(k):
        for j in range(H // CB if H >= CB else 1):
            cols = pl.ds(j * CB, min(CB, H))
            total = None
            for b, xx in ((0, xo), (1, xp)):
                part = lax.dot_general(dwb[b], xx[k, cols, :], (((1,), (1,)), ((), ())),
                                       preferred_element_type=jnp.float32)
                part = part.astype(jnp.bfloat16).astype(jnp.float32)
                total = part if total is None else total + part
            pf[k, :, cols] = total[:KP]

    def gradient(k):
        rows = gat[k]
        for b, xx in ((0, xo), (1, xp)):
            for j in range(DP // CB):
                cols = pl.ds(j * CB, CB)
                part = jnp.dot(rows, xx[k, :, cols], preferred_element_type=jnp.float32)
                g[b, :, cols] += part[:KP]

    def rs_up(m, src):
        return Split(lambda q: remote(src.at[rows32[q]], rup.at[m, rows32[q]], rsu_s.at[m], rsu_r.at[m], up))

    def rs_dn(m, src):
        return Split(lambda q: remote(src.at[rows32[q]], rdn.at[m, rows32[q]], rsd_s.at[m], rsd_r.at[m], dn))

    def ring_step(m, t, with_recv, with_send):
        ku, kd = up_chunk(m), dn_chunk(m)

        @pl.when(t == 0)
        def _():
            for k in (ku, kd):
                xo_copy(k).wait()
                xp_copy(k).wait_recv()
        product(ku)
        if with_send and not with_recv:
            rs_up(m, pf.at[ku]).start()
        product(kd)
        if with_send and not with_recv:
            rs_dn(m, pf.at[kd]).start()
        if with_recv:
            s = m - 2
            rs_up(s, rup.at[s]).wait_recv()
            rup[s] += pf[ku]
            rs_up(m, rup.at[s]).start()
            rs_dn(s, rdn.at[s]).wait_recv()
            rdn[s] += pf[kd]
            rs_dn(m, rdn.at[s]).start()

    def reduce_round(t):
        def first(m, _):
            ring_step(m, t, False, True)
            return 0

        def rest(m, _):
            ring_step(m, t, True, True)

            @pl.when((t == 0) & (m == STAGGER) & (c == 0))
            def _():
                pl.semaphore_signal(go_sem, inc=1, device_id=pal, device_id_type=MESH)
            return 0
        lax.fori_loop(0, 2, first, 0)
        lax.fori_loop(2, hops, rest, 0)
        ring_step(hops, t, False, False)
        g[...] = jnp.zeros_like(g)
        a, b = hops - 2, hops - 1
        rs_up(a, rup.at[a]).wait_recv()
        rs_dn(a, rdn.at[a]).wait_recv()
        rs_up(b, rup.at[b]).wait_recv()
        k0, k1 = chunk(0, 0), chunk(0, 1)
        res[0] = res[0] - (rup[b] + rdn[a] + pf[k0])
        rs_dn(b, rdn.at[b]).wait_recv()
        res[1] = res[1] - (rup[a] + rdn[b] + pf[k1])

        def drain(m, _):
            rs_up(m, rup.at[m]).wait_send()
            rs_dn(m, rdn.at[m]).wait_send()
            return 0
        lax.fori_loop(0, hops, drain, 0)

    def gather_ring(buf, rows, us, ur, ds, dr, seen):
        def send_up(m, k):
            return Split(lambda q: remote(buf.at[k, rows[q]], buf.at[k, rows[q]], us.at[m], ur.at[m], up))

        def send_dn(m, k):
            return Split(lambda q: remote(buf.at[k, rows[q]], buf.at[k, rows[q]], ds.at[m], dr.at[m], dn))
        k0, k1 = chunk(0, 0), chunk(0, 1)
        send_up(0, k0).start()
        send_dn(0, k1).start()
        send_up(1, k1).start()
        send_dn(1, k0).start()
        seen(k0)
        seen(k1)

        def step(m, _):
            far = lax.div(m, 2) + 1
            ku, kd = chunk(-far, lax.rem(m, 2)), chunk(far, 1 - lax.rem(m, 2))
            send_up(m, ku).wait_recv()

            @pl.when(m < hops - 2)
            def _():
                send_up(m + 2, ku).start()
            send_dn(m, kd).wait_recv()

            @pl.when(m < hops - 2)
            def _():
                send_dn(m + 2, kd).start()
            seen(ku)
            seen(kd)
            return 0
        lax.fori_loop(0, hops, step, 0)

        def drain(m, _):
            send_up(m, k0).wait_send()
            send_dn(m, k0).wait_send()
            return 0
        lax.fori_loop(0, hops, drain, 0)

    first = lax.broadcasted_iota(jnp.int32, (KP, 1), 0) + c * KS < K
    lam = jnp.where(first, jnp.float32(LAMS[0]), jnp.float32(LAMS[1]))

    def one_round(t, _):
        reduce_round(t)

        @pl.when(t < SWEEPS)
        def _():
            for h in range(2):
                gat[chunk(0, h)] = to_half(res[h])
            gather_ring(gat, rows16, agu_s, agu_r, agd_s, agd_r, gradient)
            for b in range(2):
                for j in range(DP // CB):
                    cols = pl.ds(j * CB, CB)
                    old = w[b, :, cols]
                    step = eta[b, :, cols] * (g[b, :, cols] * (1.0 / N) - lam * old)
                    w[b, :, cols] = old + step
                    dwb[b, :, cols] = to_half(step)
        return 0

    lax.fori_loop(0, SWEEPS + 1, one_round, 0)

    def w_own_copy(q):
        return local(w.at[0, rows32[q]], w_res.at[rows_out[q]], wo_sem.at[0])

    def w_pal_copy(q):
        return remote(w.at[1, rows32[q]], w_res.at[rows_out[q]], wo_sem.at[1], wo_sem.at[2], pal)
    w_own, w_pal = Split(w_own_copy), Split(w_pal_copy)
    w_own.start()
    w_pal.start()
    for h in range(2):
        rf[chunk(0, h)] = res[h]

    def out_local(k):
        return Split(lambda q: local(rf.at[k, rows32[q]], r_res.at[k, rows_out[q]], lo_s.at[k]))

    def out_pal(k):
        return Split(lambda q: out_pal_copy(k, q))

    def out_pal_copy(k, q):
        return remote(rf.at[k, rows32[q]], r_res.at[k, rows_out[q]], po_s.at[k], po_r.at[k], pal)

    def emit(k):
        out_pal(k).start()
        out_local(k).start()
    gather_ring(rf, rows32, fgu_s, fgu_r, fgd_s, fgd_r, emit)

    def finish(k, _):
        out_local(k).wait()
        out_pal(k).wait_send()
        Split(lambda q: out_pal_copy(k, 1 - q)).wait_recv()
        xp_copy(k).wait_send()
        return 0
    lax.fori_loop(0, 2 * Z, finish, 0)
    w_own.wait()
    w_pal.do(lambda cp: cp.wait_send())
    Split(lambda q: w_pal_copy(1 - q)).wait_recv()


def _fused(x, wt, eta, yt, cfg):
    Z, KS, KP, KB, H, DP, N = cfg
    K = wt.shape[0]
    hops = Z - 1
    any_spec = pl.BlockSpec(memory_space=pl.ANY)
    f32, b16 = jnp.float32, jnp.bfloat16
    dma = pltpu.SemaphoreType.DMA
    scratch = [
        pltpu.VMEM((2 * Z, H, DP), b16), pltpu.VMEM((2 * Z, H, DP), b16),
        pltpu.VMEM((2 * Z, KP, H), f32),
        pltpu.VMEM((hops, KP, H), f32), pltpu.VMEM((hops, KP, H), f32),
        pltpu.VMEM((2 * Z, KB, H), b16),
        pltpu.VMEM((2, KP, DP), f32), pltpu.VMEM((2, KP, DP), f32), pltpu.VMEM((2, KB, DP), b16),
        pltpu.VMEM((2, 1, DP), f32), pltpu.VMEM((2, KP, H), f32),
        pltpu.VMEM((2 * Z, KP, H), f32),
        dma((2 * Z,)), dma((2 * Z,)), dma((2 * Z,)), dma((7,)),
    ] + [dma((hops,))] * 12 + [dma((2 * Z,)), dma((2 * Z,)), dma((2 * Z,)), dma((3,))] + [
        pltpu.VMEM((2, K, 2, DP), f32), pltpu.VMEM((K, 2, 2 * H), f32),
        pltpu.VMEM((2 * K, max(DP, 2 * H)), f32), pltpu.SemaphoreType.REGULAR,
    ]
    flops = (SWEEPS * 2 + 1) * 2 * N * DP * 2 * KP
    return pl.pallas_call(
        functools.partial(_kernel, cfg),
        out_shape=(jax.ShapeDtypeStruct((2 * K, DP), f32), jax.ShapeDtypeStruct((2 * Z, 2 * K, H), f32)),
        in_specs=[any_spec] * 4,
        out_specs=(any_spec, any_spec),
        scratch_shapes=scratch,
        compiler_params=pltpu.CompilerParams(collective_id=0, has_side_effects=True, vmem_limit_bytes=64000000),
        cost_estimate=pl.CostEstimate(flops=flops, bytes_accessed=2 * N * DP * 2, transcendentals=0),
    )(x, wt, eta, yt)


def _arrange_kernel(K, H, w_flat, r_flat, w_new, r_new):
    @pl.when(pl.program_id(0) == 0)
    def _():
        for q in range(2):
            w_new[:, q, :] = w_flat[q * K:(q + 1) * K]
    for i in range(r_flat.shape[0]):
        for q in range(2):
            r_new[:, q, i * H:(i + 1) * H] = r_flat[i, q * K:(q + 1) * K]


def _arrange(w_flat, r_flat):
    K2, DP = w_flat.shape
    chunks, _, H = r_flat.shape
    K, per = K2 // 2, 2
    f32 = jnp.float32
    return pl.pallas_call(
        functools.partial(_arrange_kernel, K, H),
        grid=(chunks // per,),
        in_specs=[pl.BlockSpec((K2, DP), lambda i: (0, 0)), pl.BlockSpec((per, K2, H), lambda i: (i, 0, 0))],
        out_specs=(pl.BlockSpec((K, 2, DP), lambda i: (0, 0, 0)), pl.BlockSpec((K, 2, per * H), lambda i: (0, 0, i))),
        out_shape=(jax.ShapeDtypeStruct((K, 2, DP), f32), jax.ShapeDtypeStruct((K, 2, chunks * H), f32)),
    )(w_flat, r_flat)


def solution(mesh):
    Z = mesh.shape["feat"] // 2

    def per_device(x_blk, w_blk, y_blk, eta_blk):
        N, DP = x_blk.shape
        K = y_blk.shape[2]
        KS = K // 16 * 16
        KP = 2 * K - KS
        KB = -(-KP // 16) * 16
        H = N // (2 * Z)
        cfg = (Z, KS, KP, KB, H, DP, N)
        wt = jnp.transpose(w_blk, (2, 1, 0))
        yt = jnp.transpose(y_blk, (2, 1, 0))
        w_flat, r_flat = _fused(x_blk.reshape(2 * Z, H, DP), wt, eta_blk.reshape(1, DP), yt, cfg)
        w_new, r_new = _arrange(w_flat, r_flat)
        return jnp.transpose(w_new, (2, 1, 0)), jnp.transpose(r_new, (2, 1, 0))

    x_spec = P("prob", "feat")
    w_spec = P(("prob", "feat"), None, None)
    y_spec = P("prob", None, None)
    e_spec = P(("prob", "feat"))
    return jax.shard_map(per_device, mesh=mesh, in_specs=(x_spec, w_spec, y_spec, e_spec),
                         out_specs=(w_spec, y_spec), check_vma=False)
```

```python
import functools

import jax
import jax.numpy as jnp
from jax import lax
from jax.experimental import pallas as pl
from jax.experimental.pallas import tpu as pltpu
from jax.sharding import PartitionSpec as P

SWEEPS = 4
LAMS = (0.1, 1.0)
PIECES = 2
MESH = pl.DeviceIdType.MESH


def _kernel(cfg, x_in, w_in, eta_in, y_in, w_res, r_res,
            xo, xp, pf, rup, rdn, gat, w, g, dwb, eta, res, rf,
            xo_sem, xs_sem, xr_sem, in_sem,
            rsu_s, rsu_r, rsd_s, rsd_r,
            agu_s, agu_r, agd_s, agd_r,
            fgu_s, fgu_r, fgd_s, fgd_r,
            po_s, po_r, lo_s, wo_sem, raw, yraw, flat):
    Z, KS, KP, KB, H, DP, N = cfg
    K = w_in.shape[0]
    hops = Z - 1
    half_ring = Z // 2
    me = lax.axis_index("feat")
    z = lax.div(me, 2)
    c = lax.rem(me, 2)
    up = {"feat": lax.rem(z + 1, Z) * 2 + c}
    dn = {"feat": lax.rem(z + Z - 1, Z) * 2 + c}
    pal = {"feat": me + 1 - 2 * c}

    def chunk(off, half):
        return lax.rem(z + off + Z, Z) * 2 + half

    def up_chunk(m):
        return chunk(half_ring - lax.div(m + 1, 2), lax.rem(m, 2))

    def dn_chunk(m):
        return chunk(lax.div(m + 1, 2) - half_ring, 1 - lax.rem(m, 2))

    def remote(src, dst, ss, rs, dev):
        return pltpu.make_async_remote_copy(src_ref=src, dst_ref=dst, send_sem=ss, recv_sem=rs,
                                            device_id=dev, device_id_type=MESH)

    class Split:
        def __init__(self, make):
            self.make = make

        def do(self, act):
            @pl.when(c == 0)
            def _():
                act(self.make(0))

            @pl.when(c == 1)
            def _():
                act(self.make(1))

        def start(self):
            self.do(lambda cp: cp.start())

        def wait(self):
            self.do(lambda cp: cp.wait())

        def wait_send(self):
            self.do(lambda cp: cp.wait_send())

        def wait_recv(self):
            self.do(lambda cp: cp.wait_recv())

    rows32 = (pl.ds(0, KS), pl.ds(0, KP))
    rows16 = (pl.ds(0, KS), pl.ds(0, KB))
    piece = H // PIECES
    lanes = [pl.ds(i * piece, piece) for i in range(PIECES)]
    rows_out = (pl.ds(0, KS), pl.ds(KS, KP))

    local = pltpu.make_async_copy

    y_cols = pl.ds(pl.multiple_of(z * (2 * H), 2 * H), 2 * H)
    in_copies = [local(w_in, raw.at[0], in_sem.at[0]),
                 local(eta_in, eta.at[0], in_sem.at[1]),
                 local(y_in.at[:, :, y_cols], yraw, in_sem.at[2])]
    for cp in in_copies:
        cp.start()

    def xo_copy(k):
        return local(x_in.at[k], xo.at[k], xo_sem.at[k])

    def xp_copy(k):
        return remote(x_in.at[k], xp.at[k], xs_sem.at[k], xr_sem.at[k], pal)

    def start_xo(m, _):
        xo_copy(up_chunk(m)).start()
        xo_copy(dn_chunk(m)).start()
        return 0
    lax.fori_loop(0, Z, start_xo, 0)

    bar = pltpu.get_barrier_semaphore()
    for dev in (up, dn, pal):
        pl.semaphore_signal(bar, inc=1, device_id=dev, device_id_type=MESH)
    pl.semaphore_wait(bar, 3)

    w_x = remote(w_in, raw.at[1], in_sem.at[3], in_sem.at[4], pal)
    e_x = remote(eta_in, eta.at[1], in_sem.at[5], in_sem.at[6], pal)
    w_x.start()
    e_x.start()

    def start_xp(m, _):
        xp_copy(up_chunk(m)).start()
        xp_copy(dn_chunk(m)).start()
        return 0
    lax.fori_loop(0, Z, start_xp, 0)

    for cp in in_copies:
        cp.wait()
    w_x.wait()
    e_x.wait()

    def to_half(v):
        return jnp.concatenate([v, jnp.zeros((KB - KP, v.shape[1]), jnp.float32)], axis=0).astype(jnp.bfloat16)

    mine = pl.ds(pl.multiple_of(c * KS, 8), KP)

    def flatten(src):
        wide = src.shape[2]
        flat[0:K, 0:wide] = src[:, 0, :]
        flat[K:2 * K, 0:wide] = src[:, 1, :]

    for b in range(2):
        flatten(raw.at[b])
        w[b] = flat[mine, 0:DP]
        dwb[b] = to_half(w[b])
    flatten(yraw)
    for h in range(2):
        res[h] = flat[mine, h * H:(h + 1) * H]

    CB = 256

    def product(k):
        for j in range(H // CB if H >= CB else 1):
            cols = pl.ds(j * CB, min(CB, H))
            total = None
            for b, xx in ((0, xo), (1, xp)):
                part = lax.dot_general(dwb[b], xx[k, cols, :], (((1,), (1,)), ((), ())),
                                       preferred_element_type=jnp.float32)
                part = part.astype(jnp.bfloat16).astype(jnp.float32)
                total = part if total is None else total + part
            pf[k, :, cols] = total[:KP]

    def gradient(k):
        rows = gat[k]
        for b, xx in ((0, xo), (1, xp)):
            for j in range(DP // CB):
                cols = pl.ds(j * CB, CB)
                part = jnp.dot(rows, xx[k, :, cols], preferred_element_type=jnp.float32)
                g[b, :, cols] += part[:KP]

    def rs_up(m, src, i):
        s = m * PIECES + i
        return Split(lambda q: remote(src.at[rows32[q], lanes[i]], rup.at[m, rows32[q], lanes[i]],
                                      rsu_s.at[s], rsu_r.at[s], up))

    def rs_dn(m, src, i):
        s = m * PIECES + i
        return Split(lambda q: remote(src.at[rows32[q], lanes[i]], rdn.at[m, rows32[q], lanes[i]],
                                      rsd_s.at[s], rsd_r.at[s], dn))

    def ring_step(m, t, with_recv, with_send):
        ku, kd = up_chunk(m), dn_chunk(m)

        @pl.when(t == 0)
        def _():
            for k in (ku, kd):
                xo_copy(k).wait()
                xp_copy(k).wait_recv()
        product(ku)
        if with_send and not with_recv:
            for i in range(PIECES):
                rs_up(m, pf.at[ku], i).start()
        product(kd)
        if with_send and not with_recv:
            for i in range(PIECES):
                rs_dn(m, pf.at[kd], i).start()
        if with_recv:
            s = m - 2
            for i in range(PIECES):
                rs_up(s, rup.at[s], i).wait_recv()
                rup[s, :, lanes[i]] += pf[ku, :, lanes[i]]
                rs_up(m, rup.at[s], i).start()
                rs_dn(s, rdn.at[s], i).wait_recv()
                rdn[s, :, lanes[i]] += pf[kd, :, lanes[i]]
                rs_dn(m, rdn.at[s], i).start()

    def reduce_round(t):
        def first(m, _):
            ring_step(m, t, False, True)
            return 0

        def rest(m, _):
            ring_step(m, t, True, True)
            return 0
        lax.fori_loop(0, 2, first, 0)
        lax.fori_loop(2, hops, rest, 0)
        ring_step(hops, t, False, False)
        g[...] = jnp.zeros_like(g)
        a, b = hops - 2, hops - 1
        for i in range(PIECES):
            rs_up(a, rup.at[a], i).wait_recv()
            rs_dn(a, rdn.at[a], i).wait_recv()
        for i in range(PIECES):
            rs_up(b, rup.at[b], i).wait_recv()
        k0, k1 = chunk(0, 0), chunk(0, 1)
        res[0] = res[0] - (rup[b] + rdn[a] + pf[k0])
        for i in range(PIECES):
            rs_dn(b, rdn.at[b], i).wait_recv()
        res[1] = res[1] - (rup[a] + rdn[b] + pf[k1])

        def drain(m, _):
            for i in range(PIECES):
                rs_up(m, rup.at[m], i).wait_send()
                rs_dn(m, rdn.at[m], i).wait_send()
            return 0
        lax.fori_loop(0, hops, drain, 0)

    def gather_ring(buf, rows, us, ur, ds, dr, seen):
        def send_up(m, k, i):
            s = m * PIECES + i
            return Split(lambda q: remote(buf.at[k, rows[q], lanes[i]], buf.at[k, rows[q], lanes[i]],
                                          us.at[s], ur.at[s], up))

        def send_dn(m, k, i):
            s = m * PIECES + i
            return Split(lambda q: remote(buf.at[k, rows[q], lanes[i]], buf.at[k, rows[q], lanes[i]],
                                          ds.at[s], dr.at[s], dn))
        k0, k1 = chunk(0, 0), chunk(0, 1)
        for m, ku, kd in ((0, k0, k1), (1, k1, k0)):
            for i in range(PIECES):
                send_up(m, ku, i).start()
                send_dn(m, kd, i).start()
        seen(k0)
        seen(k1)

        def step(m, _):
            far = lax.div(m, 2) + 1
            ku, kd = chunk(-far, lax.rem(m, 2)), chunk(far, 1 - lax.rem(m, 2))
            for i in range(PIECES):
                send_up(m, ku, i).wait_recv()

                @pl.when(m < hops - 2)
                def _():
                    send_up(m + 2, ku, i).start()
                send_dn(m, kd, i).wait_recv()

                @pl.when(m < hops - 2)
                def _():
                    send_dn(m + 2, kd, i).start()
            seen(ku)
            seen(kd)
            return 0
        lax.fori_loop(0, hops, step, 0)

        def drain(m, _):
            for i in range(PIECES):
                send_up(m, k0, i).wait_send()
                send_dn(m, k0, i).wait_send()
            return 0
        lax.fori_loop(0, hops, drain, 0)

    first = lax.broadcasted_iota(jnp.int32, (KP, 1), 0) + c * KS < K
    lam = jnp.where(first, jnp.float32(LAMS[0]), jnp.float32(LAMS[1]))

    def one_round(t, _):
        reduce_round(t)

        @pl.when(t < SWEEPS)
        def _():
            for h in range(2):
                gat[chunk(0, h)] = to_half(res[h])
            gather_ring(gat, rows16, agu_s, agu_r, agd_s, agd_r, gradient)
            for b in range(2):
                for j in range(DP // CB):
                    cols = pl.ds(j * CB, CB)
                    old = w[b, :, cols]
                    step = eta[b, :, cols] * (g[b, :, cols] * (1.0 / N) - lam * old)
                    w[b, :, cols] = old + step
                    dwb[b, :, cols] = to_half(step)
        return 0

    lax.fori_loop(0, SWEEPS + 1, one_round, 0)

    def w_own_copy(q):
        return local(w.at[0, rows32[q]], w_res.at[rows_out[q]], wo_sem.at[0])

    def w_pal_copy(q):
        return remote(w.at[1, rows32[q]], w_res.at[rows_out[q]], wo_sem.at[1], wo_sem.at[2], pal)
    w_own, w_pal = Split(w_own_copy), Split(w_pal_copy)
    w_own.start()
    w_pal.start()
    for h in range(2):
        rf[chunk(0, h)] = res[h]

    def out_local(k):
        return Split(lambda q: local(rf.at[k, rows32[q]], r_res.at[k, rows_out[q]], lo_s.at[k]))

    def out_pal(k):
        return Split(lambda q: out_pal_copy(k, q))

    def out_pal_copy(k, q):
        return remote(rf.at[k, rows32[q]], r_res.at[k, rows_out[q]], po_s.at[k], po_r.at[k], pal)

    def emit(k):
        out_pal(k).start()
        out_local(k).start()
    gather_ring(rf, rows32, fgu_s, fgu_r, fgd_s, fgd_r, emit)

    def finish(k, _):
        out_local(k).wait()
        out_pal(k).wait_send()
        Split(lambda q: out_pal_copy(k, 1 - q)).wait_recv()
        xp_copy(k).wait_send()
        return 0
    lax.fori_loop(0, 2 * Z, finish, 0)
    w_own.wait()
    w_pal.do(lambda cp: cp.wait_send())
    Split(lambda q: w_pal_copy(1 - q)).wait_recv()


def _fused(x, wt, eta, yt, cfg):
    Z, KS, KP, KB, H, DP, N = cfg
    K = wt.shape[0]
    hops = Z - 1
    any_spec = pl.BlockSpec(memory_space=pl.ANY)
    f32, b16 = jnp.float32, jnp.bfloat16
    dma = pltpu.SemaphoreType.DMA
    scratch = [
        pltpu.VMEM((2 * Z, H, DP), b16), pltpu.VMEM((2 * Z, H, DP), b16),
        pltpu.VMEM((2 * Z, KP, H), f32),
        pltpu.VMEM((hops, KP, H), f32), pltpu.VMEM((hops, KP, H), f32),
        pltpu.VMEM((2 * Z, KB, H), b16),
        pltpu.VMEM((2, KP, DP), f32), pltpu.VMEM((2, KP, DP), f32), pltpu.VMEM((2, KB, DP), b16),
        pltpu.VMEM((2, 1, DP), f32), pltpu.VMEM((2, KP, H), f32),
        pltpu.VMEM((2 * Z, KP, H), f32),
        dma((2 * Z,)), dma((2 * Z,)), dma((2 * Z,)), dma((7,)),
    ] + [dma((hops * PIECES,))] * 12 + [dma((2 * Z,)), dma((2 * Z,)), dma((2 * Z,)), dma((3,))] + [
        pltpu.VMEM((2, K, 2, DP), f32), pltpu.VMEM((K, 2, 2 * H), f32),
        pltpu.VMEM((2 * K, max(DP, 2 * H)), f32),
    ]
    flops = (SWEEPS * 2 + 1) * 2 * N * DP * 2 * KP
    return pl.pallas_call(
        functools.partial(_kernel, cfg),
        out_shape=(jax.ShapeDtypeStruct((2 * K, DP), f32), jax.ShapeDtypeStruct((2 * Z, 2 * K, H), f32)),
        in_specs=[any_spec] * 4,
        out_specs=(any_spec, any_spec),
        scratch_shapes=scratch,
        compiler_params=pltpu.CompilerParams(collective_id=0, has_side_effects=True, vmem_limit_bytes=64000000),
        cost_estimate=pl.CostEstimate(flops=flops, bytes_accessed=2 * N * DP * 2, transcendentals=0),
    )(x, wt, eta, yt)


def _arrange_kernel(K, H, w_flat, r_flat, w_new, r_new, w_a, r_a, w_b, r_b, sem_a, sem_b):
    chunks = r_flat.shape[0]
    local = pltpu.make_async_copy

    def load(i):
        return local(r_flat.at[i], r_a.at[i], sem_a.at[i])

    def store(i):
        cols = pl.ds(pl.multiple_of(i * H, H), H)
        return local(r_b.at[i], r_new.at[:, :, cols], sem_b.at[i])
    w_load = local(w_flat, w_a, sem_a.at[chunks])
    w_store = local(w_b, w_new, sem_b.at[chunks])
    w_load.start()

    def begin(i, _):
        load(i).start()
        return 0
    lax.fori_loop(0, chunks, begin, 0)
    w_load.wait()
    for q in range(2):
        w_b[:, q, :] = w_a[q * K:(q + 1) * K]
    w_store.start()

    def move(i, _):
        load(i).wait()
        for q in range(2):
            r_b[i, :, q, :] = r_a[i, q * K:(q + 1) * K]
        store(i).start()
        return 0
    lax.fori_loop(0, chunks, move, 0)

    def end(i, _):
        store(i).wait()
        return 0
    lax.fori_loop(0, chunks, end, 0)
    w_store.wait()


def _arrange(w_flat, r_flat):
    K2, DP = w_flat.shape
    chunks, _, H = r_flat.shape
    K = K2 // 2
    f32 = jnp.float32
    any_spec = pl.BlockSpec(memory_space=pl.ANY)
    return pl.pallas_call(
        functools.partial(_arrange_kernel, K, H),
        in_specs=[any_spec, any_spec],
        out_specs=(any_spec, any_spec),
        out_shape=(jax.ShapeDtypeStruct((K, 2, DP), f32), jax.ShapeDtypeStruct((K, 2, chunks * H), f32)),
        scratch_shapes=[pltpu.VMEM((K2, DP), f32), pltpu.VMEM((chunks, K2, H), f32),
                        pltpu.VMEM((K, 2, DP), f32), pltpu.VMEM((chunks, K, 2, H), f32),
                        pltpu.SemaphoreType.DMA((chunks + 1,)), pltpu.SemaphoreType.DMA((chunks + 1,))],
        compiler_params=pltpu.CompilerParams(vmem_limit_bytes=64000000),
    )(w_flat, r_flat)


def solution(mesh):
    Z = mesh.shape["feat"] // 2

    def per_device(x_blk, w_blk, y_blk, eta_blk):
        N, DP = x_blk.shape
        K = y_blk.shape[2]
        KS = K // 16 * 16
        KP = 2 * K - KS
        KB = -(-KP // 16) * 16
        H = N // (2 * Z)
        cfg = (Z, KS, KP, KB, H, DP, N)
        wt = jnp.transpose(w_blk, (2, 1, 0))
        yt = jnp.transpose(y_blk, (2, 1, 0))
        w_flat, r_flat = _fused(x_blk.reshape(2 * Z, H, DP), wt, eta_blk.reshape(1, DP), yt, cfg)
        w_new, r_new = _arrange(w_flat, r_flat)
        return jnp.transpose(w_new, (2, 1, 0)), jnp.transpose(r_new, (2, 1, 0))

    x_spec = P("prob", "feat")
    w_spec = P(("prob", "feat"), None, None)
    y_spec = P("prob", None, None)
    e_spec = P(("prob", "feat"))
    return jax.shard_map(per_device, mesh=mesh, in_specs=(x_spec, w_spec, y_spec, e_spec),
                         out_specs=(w_spec, y_spec), check_vma=False)
```
